32 devices in a mesh: py: 4 (over y, x), pz: 8 (over z, core).
Axes of the slice: x: 2, y: 2, z: 4, core: 2. Of those that a mesh axis runs over, the one named last changes fastest.
Arguments:
- species: float32 [4, 512, 64, 64], P(None, None, 'py', 'pz'), may hold values from -6 to 6
- coupling: float32 [4, 4], replicated, may hold values from -4 to 4
- symbol_x: float32 [512], replicated, may hold values from 0.3 to 3
- symbol_y: float32 [64], replicated, may hold values from 0.3 to 3
- symbol_z: float32 [64], replicated, may hold values from 0.3 to 3
Outputs:
- modes: float32 [4, 512, 64, 64], P(None, 'py', 'pz')
The draws below stay inside these ranges and needn't reach their ends.
All inputs are finite; a program needn't handle non-finite values.
Results may differ from the reference program's by a relative error of at most 0.00007.
Values sent between devices are 32-bit elements; how exact they have to be, the bound alone decides.
A program may use at most 64 MiB of HBM per device.

```python
import jax
import jax.numpy as jnp
from jax import lax

GRID_X = 512
GRID_Y = 64
GRID_Z = 64
FIELDS = 4


def block_levels(key, shape, pieces, low, largest):
    def one(dim, shards_of):
        draws = jax.random.uniform(jax.random.fold_in(jax.random.fold_in(key, 6), dim), (shards_of,), jnp.float32, low / len(pieces), largest / len(pieces))
        return jnp.repeat(jnp.exp(draws), shape[dim] // shards_of).reshape((-1,) + (1,) * (len(shape) - dim - 1))

    gain = one(*pieces[0])
    for cut in pieces[1:]:
        gain = gain * one(*cut)
    return gain


def bell_draw(rng, shape, spread, most, shards=(), dtype=jnp.bfloat16):
    result = spread * jax.random.normal(rng, shape, jnp.float32)
    if shards:
        result = result * block_levels(rng, shape, shards, -0.22, 0.18)
    return jnp.clip(result, -most, most).astype(dtype)


def setup_inputs(seed: int = 0) -> dict:
    key_list = jax.random.split(jax.random.key(seed), 6)
    return {
        "species": bell_draw(key_list[0], (FIELDS, GRID_X, GRID_Y, GRID_Z), 1.0, 6.0, ((2, 4), (3, 8)), jnp.float32),
        "coupling": bell_draw(key_list[1], (FIELDS, FIELDS), 0.7, 4.0, (), jnp.float32),
        "symbol_x": jnp.clip(jax.random.uniform(key_list[2], (GRID_X,), jnp.float32, 0.3, 3.0), 0.3, 3.0),
        "symbol_y": jnp.clip(jax.random.uniform(key_list[3], (GRID_Y,), jnp.float32, 0.3, 3.0), 0.3, 3.0),
        "symbol_z": jnp.clip(jax.random.uniform(key_list[4], (GRID_Z,), jnp.float32, 0.3, 3.0), 0.3, 3.0),
    }


def mode_table(count):
    rank = jnp.arange(count)
    angle = (jnp.pi / (4 * count)) * (((2 * rank[:, None] + 1) * (2 * rank[None, :] + 1)) % (8 * count)).astype(jnp.float32)
    return jnp.cos(angle) * (2.0 / count) ** 0.5


def transform_dim(values, dim):
    moved = jnp.tensordot(values, mode_table(values.shape[dim]), axes=([dim], [0]), precision=lax.Precision.HIGHEST)
    return jnp.moveaxis(moved, -1, dim)


def reference(species, coupling, symbol_x, symbol_y, symbol_z):
    modes = species
    modes = transform_dim(modes, 1)
    modes = transform_dim(modes, 2)
    modes = transform_dim(modes, 3)
    symbol = symbol_x[:, None, None] + symbol_y[None, :, None] + symbol_z[None, None, :]
    weight_xyz = 1.0 / (1.0 + symbol)
    mixed_fields = jnp.einsum("ab,bxyz->axyz", coupling, modes, precision=lax.Precision.HIGHEST)
    modes = weight_xyz * modes + (1.0 - weight_xyz) * mixed_fields
    return modes
```

```python
import functools

import jax
import jax.numpy as jnp
import numpy as np
from jax import lax
from jax.experimental import pallas as pl
from jax.experimental.pallas import tpu as pltpu
from jax.sharding import PartitionSpec as P

MESH = pl.DeviceIdType.MESH
F32 = jnp.float32
BF16 = jnp.bfloat16
LANES, SUBLANES = 128, 8
VMEM_BUDGET = 48 << 20


def mode_table(count):
    rank = jnp.arange(count)
    angle = (
        jnp.pi
        / (4 * count)
        * ((2 * rank[:, None] + 1) * (2 * rank[None, :] + 1) % (8 * count)).astype(jnp.float32)
    )
    return jnp.cos(angle) * (2.0 / count) ** 0.5


def transform_dim(values, dim):
    moved = jnp.tensordot(
        values, mode_table(values.shape[dim]), axes=([dim], [0]), precision=lax.Precision.HIGHEST
    )
    return jnp.moveaxis(moved, -1, dim)


def plain_shards(species, coupling, symbol_x, symbol_y, symbol_z):
    values = transform_dim(species, 1)
    values = lax.all_to_all(values, "py", split_axis=1, concat_axis=2, tiled=True)
    values = transform_dim(values, 2)
    values = lax.all_to_all(values, "pz", split_axis=2, concat_axis=3, tiled=True)
    values = transform_dim(values, 3)
    share_x = values.shape[1]
    part_x = lax.dynamic_slice_in_dim(symbol_x, lax.axis_index("py") * share_x, share_x)
    share_y = values.shape[2]
    part_y = lax.dynamic_slice_in_dim(symbol_y, lax.axis_index("pz") * share_y, share_y)
    symbol = part_x[:, None, None] + part_y[None, :, None] + symbol_z[None, None, :]
    weight = 1.0 / (1.0 + symbol)
    mixed = jnp.einsum("ab,bxyz->axyz", coupling, values, precision=lax.Precision.HIGHEST)
    return weight * values + (1.0 - weight) * mixed


def split_table(count):
    rank = 2 * np.arange(count) + 1
    table = np.cos(np.pi / (4 * count) * (rank[:, None] * rank[None, :] % (8 * count)))
    table = (table * np.sqrt(2.0 / count)).astype(np.float32)
    high = table.astype(BF16)
    low = (table - high.astype(np.float32)).astype(BF16)
    return np.stack([high, low])


def split(values):
    high = values.astype(BF16)
    low = (values - high.astype(F32)).astype(BF16)
    return high, low


def dot(a, b):
    return jnp.dot(a, b, preferred_element_type=F32)


def flipped(index, offset, count):
    if count & (count - 1):
        return lax.rem(index + offset, count)
    result = index
    bit = 1
    while bit < count:
        if offset & bit:
            result = result + bit - 2 * bit * lax.rem(index // bit, 2)
        bit *= 2
    return result


def source_of(index, offset, count):
    if count & (count - 1):
        return lax.rem(index + count - offset, count)
    return flipped(index, offset, count)


def kernel(
    dims, field_ref, hx_hbm, hy_ref, hz_ref, coupling_ref, sx_ref, sy_ref, sz_ref, out_ref,
    held, hx, lines_out, lines, parts_out, parts, modes, my, mz,
    load_sem, hx_sem, send_y, recv_y, send_z, recv_z,
):
    fields, ny, nz, n_py, n_pz, yl, zl, share_x, share_y = dims
    py, pz = lax.axis_index("py"), lax.axis_index("pz")
    rows_y = yl * zl
    rows_z = share_y * zl
    depth_y = ny * zl
    rows_out = share_y * nz
    depth_z = n_pz * rows_z

    def load(f):
        return pltpu.make_async_copy(field_ref.at[f], held.at[f], load_sem.at[f])

    hx_copy = pltpu.make_async_copy(hx_hbm, hx, hx_sem)
    load(0).start()
    hx_copy.start()
    for f in range(1, fields):
        load(f).start()
    barrier = pltpu.get_barrier_semaphore()
    for o in range(1, n_pz):
        pl.semaphore_signal(
            barrier, inc=1, device_id={"pz": flipped(pz, o, n_pz)}, device_id_type=MESH
        )
    for o in range(1, n_py):
        pl.semaphore_signal(
            barrier, inc=1, device_id={"py": flipped(py, o, n_py)}, device_id_type=MESH
        )

    def copy_y(f, o):
        to = flipped(py, o, n_py)
        return pltpu.make_async_remote_copy(
            src_ref=lines_out.at[f, to],
            dst_ref=lines.at[f, pl.ds(py * rows_y, rows_y)],
            send_sem=send_y.at[f, o],
            recv_sem=recv_y.at[f, o],
            device_id={"py": to},
            device_id_type=MESH,
        )

    def copy_z(f, o):
        to = flipped(pz, o, n_pz)
        return pltpu.make_async_remote_copy(
            src_ref=parts_out.at[f, pl.ds(to * rows_z, rows_z)],
            dst_ref=parts.at[f, pl.ds(pz * rows_z, rows_z)],
            send_sem=send_z.at[f, o],
            recv_sem=recv_z.at[f, o],
            device_id={"pz": to},
            device_id_type=MESH,
        )

    hx_copy.wait()
    for f in range(fields):
        load(f).wait()
        high, low = split(held[f])
        both = dot(jnp.concatenate([high, low], axis=0), hx[0])
        result = both[:rows_y] + both[rows_y:] + dot(high, hx[1])
        for d in range(n_py):
            lines_out[f, d] = result[:, d * share_x : (d + 1) * share_x]
        if f == 0:
            pl.semaphore_wait(barrier, n_py + n_pz - 2)
        for o in range(n_py - 1, 0, -1):
            copy_y(f, o).start()
        lines[f, pl.ds(py * rows_y, rows_y)] = lines_out[f, py]

    def iota(shape, dim):
        return lax.broadcasted_iota(jnp.int32, shape, dim)

    row, col = iota((depth_y, ny), 0), iota((depth_y, ny), 1)
    pick = (row // zl == col).astype(F32).astype(BF16)
    row, col = iota((ny, depth_y), 0), iota((ny, depth_y), 1)
    spread = (col // zl == row).astype(F32).astype(BF16)
    row, col = iota((depth_y, depth_y), 0), iota((depth_y, depth_y), 1)
    keep = row % zl == col % zl
    for t in range(2):
        wide = dot(dot(pick, hy_ref[t]).astype(BF16), spread)
        my[t] = jnp.where(keep, wide, 0.0).astype(BF16)
    row, col = iota((rows_out, nz), 0), iota((rows_out, nz), 1)
    pick = (row % nz == col).astype(F32).astype(BF16)
    row, col = iota((nz, depth_z), 0), iota((nz, depth_z), 1)
    spread = ((col // rows_z) * zl + col % zl == row).astype(F32).astype(BF16)
    row, col = iota((rows_out, depth_z), 0), iota((rows_out, depth_z), 1)
    keep = row // nz == (col // zl) % share_y
    for t in range(2):
        wide = dot(dot(pick, hz_ref[t]).astype(BF16), spread)
        mz[t] = jnp.where(keep, wide, 0.0).astype(BF16)

    def rows_transform(table, values):
        high, low = split(values)
        both = dot(table[0], jnp.concatenate([high, low], axis=1))
        return both[:, :share_x] + both[:, share_x:] + dot(table[1], high)

    for f in range(fields):
        for o in range(n_py - 1, 0, -1):
            copy_y(f, o).wait_recv()
        parts_out[f] = rows_transform(my, lines[f])
        for o in range(n_pz - 1, 0, -1):
            copy_z(f, o).start()
        parts[f, pl.ds(pz * rows_z, rows_z)] = parts_out[f, pl.ds(pz * rows_z, rows_z)]

    diagonal = iota((nz, nz), 0) == iota((nz, nz), 1)
    sz_column = jnp.sum(jnp.where(diagonal, sz_ref[...], 0.0), axis=1, keepdims=True)
    sx_row = sx_ref[:, pl.ds(pl.multiple_of(py * share_x, share_x), share_x)]

    for f in range(fields):
        for o in range(n_pz - 1, 0, -1):
            copy_z(f, o).wait_recv()
        modes[f] = rows_transform(mz, parts[f])
    for k in range(share_y):
        span = pl.ds(k * nz, nz)
        weight = 1.0 / (1.0 + ((sx_row + sy_ref[pz * share_y + k]) + sz_column))
        old = [modes[f, span] for f in range(fields)]
        for a in range(fields):
            mixed = coupling_ref[a, 0] * old[0]
            for b in range(1, fields):
                mixed = mixed + coupling_ref[a, b] * old[b]
            out_ref[a, span] = weight * old[a] + (1.0 - weight) * mixed
    for f in range(fields):
        for o in range(1, n_py):
            copy_y(f, o).wait_send()
        for o in range(1, n_pz):
            copy_z(f, o).wait_send()


def shards(n_py, n_pz, species, coupling, symbol_x, symbol_y, symbol_z):
    fields, nx, yl, zl = species.shape
    ny, nz = yl * n_py, zl * n_pz
    share_x, share_y = nx // n_py, ny // n_pz
    block = fields * nx * yl * zl
    tables = 2 * (nx * nx + (ny * zl) ** 2 + (share_y * nz) ** 2)
    need = 7 * 4 * block + 2 * tables + 16 * max(ny * zl, share_y * nz) ** 2
    if share_x % LANES or zl % SUBLANES or nx % n_py or ny % n_pz or need > VMEM_BUDGET:
        return plain_shards(species, coupling, symbol_x, symbol_y, symbol_z)
    dims = (fields, ny, nz, n_py, n_pz, yl, zl, share_x, share_y)
    rows_y, depth_y, depth_z = yl * zl, ny * zl, share_y * nz
    vmem = pl.BlockSpec(memory_space=pltpu.VMEM)
    smem = pl.BlockSpec(memory_space=pltpu.SMEM)
    anywhere = pl.BlockSpec(memory_space=pl.ANY)
    values = jnp.transpose(species, (0, 2, 3, 1)).reshape(fields, rows_y, nx)
    out = pl.pallas_call(
        functools.partial(kernel, dims),
        out_shape=jax.ShapeDtypeStruct((fields, depth_z, share_x), F32),
        in_specs=[anywhere, anywhere, vmem, vmem, smem, vmem, smem, vmem],
        out_specs=vmem,
        scratch_shapes=[
            pltpu.VMEM((fields, rows_y, nx), F32),
            pltpu.VMEM((2, nx, nx), BF16),
            pltpu.VMEM((fields, n_py, rows_y, share_x), F32),
            pltpu.VMEM((fields, depth_y, share_x), F32),
            pltpu.VMEM((fields, depth_y, share_x), F32),
            pltpu.VMEM((fields, depth_z, share_x), F32),
            pltpu.VMEM((fields, depth_z, share_x), F32),
            pltpu.VMEM((2, depth_y, depth_y), BF16),
            pltpu.VMEM((2, depth_z, depth_z), BF16),
            pltpu.SemaphoreType.DMA((fields,)),
            pltpu.SemaphoreType.DMA,
            pltpu.SemaphoreType.DMA((fields, n_py)),
            pltpu.SemaphoreType.DMA((fields, n_py)),
            pltpu.SemaphoreType.DMA((fields, n_pz)),
            pltpu.SemaphoreType.DMA((fields, n_pz)),
        ],
        compiler_params=pltpu.CompilerParams(
            collective_id=0, has_side_effects=True, vmem_limit_bytes=VMEM_BUDGET
        ),
    )(
        values,
        jnp.asarray(split_table(nx)),
        jnp.asarray(split_table(ny)),
        jnp.asarray(split_table(nz)),
        coupling,
        symbol_x.reshape(1, nx),
        symbol_y,
        symbol_z.reshape(1, nz),
    )
    return jnp.transpose(out.reshape(fields, share_y, nz, share_x), (0, 3, 1, 2))


def solution(mesh):
    return jax.shard_map(
        functools.partial(shards, mesh.shape["py"], mesh.shape["pz"]),
        mesh=mesh,
        in_specs=(P(None, None, "py", "pz"), P(), P(), P(), P()),
        out_specs=P(None, "py", "pz", None),
        check_vma=False,
    )
```

```python
import functools

import jax
import jax.numpy as jnp
import numpy as np
from jax import lax
from jax.experimental import pallas as pl
from jax.experimental.pallas import tpu as pltpu
from jax.sharding import PartitionSpec as P

MESH = pl.DeviceIdType.MESH
F32 = jnp.float32
BF16 = jnp.bfloat16
LANES, SUBLANES = 128, 8
VMEM_BUDGET = 48 << 20


def mode_table(count):
    rank = jnp.arange(count)
    angle = (
        jnp.pi
        / (4 * count)
        * ((2 * rank[:, None] + 1) * (2 * rank[None, :] + 1) % (8 * count)).astype(jnp.float32)
    )
    return jnp.cos(angle) * (2.0 / count) ** 0.5


def transform_dim(values, dim):
    moved = jnp.tensordot(
        values, mode_table(values.shape[dim]), axes=([dim], [0]), precision=lax.Precision.HIGHEST
    )
    return jnp.moveaxis(moved, -1, dim)


def plain_shards(species, coupling, symbol_x, symbol_y, symbol_z):
    values = transform_dim(species, 1)
    values = lax.all_to_all(values, "py", split_axis=1, concat_axis=2, tiled=True)
    values = transform_dim(values, 2)
    values = lax.all_to_all(values, "pz", split_axis=2, concat_axis=3, tiled=True)
    values = transform_dim(values, 3)
    share_x = values.shape[1]
    part_x = lax.dynamic_slice_in_dim(symbol_x, lax.axis_index("py") * share_x, share_x)
    share_y = values.shape[2]
    part_y = lax.dynamic_slice_in_dim(symbol_y, lax.axis_index("pz") * share_y, share_y)
    symbol = part_x[:, None, None] + part_y[None, :, None] + symbol_z[None, None, :]
    weight = 1.0 / (1.0 + symbol)
    mixed = jnp.einsum("ab,bxyz->axyz", coupling, values, precision=lax.Precision.HIGHEST)
    return weight * values + (1.0 - weight) * mixed


def split_table(count):
    rank = 2 * np.arange(count) + 1
    table = np.cos(np.pi / (4 * count) * (rank[:, None] * rank[None, :] % (8 * count)))
    table = (table * np.sqrt(2.0 / count)).astype(np.float32)
    high = table.astype(BF16)
    low = (table - high.astype(np.float32)).astype(BF16)
    return np.stack([high, low])


def split(values):
    high = values.astype(BF16)
    low = (values - high.astype(F32)).astype(BF16)
    return high, low


def dot(a, b):
    return jnp.dot(a, b, preferred_element_type=F32)


def flipped(index, offset, count):
    if count & (count - 1):
        return lax.rem(index + offset, count)
    result = index
    bit = 1
    while bit < count:
        if offset & bit:
            result = result + bit - 2 * bit * lax.rem(index // bit, 2)
        bit *= 2
    return result


def source_of(index, offset, count):
    if count & (count - 1):
        return lax.rem(index + count - offset, count)
    return flipped(index, offset, count)


def kernel(
    dims, field_ref, hx_hbm, hy_hbm, hz_hbm, coupling_hbm, sx_hbm, sy_hbm, sz_hbm, out_ref,
    held, hx, hy, hz, coupling, sx, sy, sz, lines_out, lines, parts_out, parts, modes, weights,
    my, mz, load_sem, side_sem, send_y, recv_y, send_z, recv_z,
):
    fields, ny, nz, n_py, n_pz, yl, zl, share_x, share_y = dims
    py, pz = lax.axis_index("py"), lax.axis_index("pz")
    rows_y = yl * zl
    rows_z = share_y * zl
    depth_y = ny * zl
    rows_out = share_y * nz
    depth_z = n_pz * rows_z

    def load(f):
        return pltpu.make_async_copy(field_ref.at[f], held.at[f], load_sem.at[f])

    pairs = (
        (hx_hbm.at[0], hx.at[0]), (hx_hbm.at[1], hx.at[1]), (hy_hbm, hy), (hz_hbm, hz),
        (coupling_hbm, coupling), (sx_hbm, sx), (sy_hbm, sy), (sz_hbm, sz),
    )
    sides = [
        pltpu.make_async_copy(a, b, side_sem.at[i]) for i, (a, b) in enumerate(pairs)
    ]
    load(0).start()
    sides[0].start()
    sides[1].start()
    for f in range(1, fields):
        load(f).start()
    for side in sides[2:]:
        side.start()
    barrier = pltpu.get_barrier_semaphore()
    for o in range(1, n_pz):
        pl.semaphore_signal(
            barrier, inc=1, device_id={"pz": flipped(pz, o, n_pz)}, device_id_type=MESH
        )
    for o in range(1, n_py):
        pl.semaphore_signal(
            barrier, inc=1, device_id={"py": flipped(py, o, n_py)}, device_id_type=MESH
        )

    def copy_y(f, o):
        to = flipped(py, o, n_py)
        return pltpu.make_async_remote_copy(
            src_ref=lines_out.at[f, to],
            dst_ref=lines.at[f, pl.ds(py * rows_y, rows_y)],
            send_sem=send_y.at[f, o],
            recv_sem=recv_y.at[f, o],
            device_id={"py": to},
            device_id_type=MESH,
        )

    def copy_z(f, o):
        to = flipped(pz, o, n_pz)
        return pltpu.make_async_remote_copy(
            src_ref=parts_out.at[f, pl.ds(to * rows_z, rows_z)],
            dst_ref=parts.at[f, pl.ds(pz * rows_z, rows_z)],
            send_sem=send_z.at[f, o],
            recv_sem=recv_z.at[f, o],
            device_id={"pz": to},
            device_id_type=MESH,
        )

    for f in range(fields):
        load(f).wait()
        high, low = split(held[f])
        if f == 0:
            sides[0].wait()
            sides[1].wait()
        both = dot(jnp.concatenate([high, low], axis=0), hx[0])
        result = both[:rows_y] + both[rows_y:] + dot(high, hx[1])
        for d in range(n_py):
            lines_out[f, d] = result[:, d * share_x : (d + 1) * share_x]
        if f == 0:
            pl.semaphore_wait(barrier, n_py + n_pz - 2)
        for o in range(n_py - 1, 0, -1):
            copy_y(f, o).start()
        lines[f, pl.ds(py * rows_y, rows_y)] = lines_out[f, py]

    for side in sides[2:]:
        side.wait()

    def iota(shape, dim):
        return lax.broadcasted_iota(jnp.int32, shape, dim)

    row, col = iota((depth_y, ny), 0), iota((depth_y, ny), 1)
    pick = (row // zl == col).astype(F32).astype(BF16)
    row, col = iota((ny, depth_y), 0), iota((ny, depth_y), 1)
    spread = (col // zl == row).astype(F32).astype(BF16)
    row, col = iota((depth_y, depth_y), 0), iota((depth_y, depth_y), 1)
    keep = row % zl == col % zl
    for t in range(2):
        wide = dot(dot(pick, hy[t]).astype(BF16), spread)
        my[t] = jnp.where(keep, wide, 0.0).astype(BF16)
    def rows_transform(high_table, low_table, high, low):
        both = dot(high_table, jnp.concatenate([high, low], axis=1))
        return both[:, :share_x] + both[:, share_x:] + dot(low_table, high)

    halves = 2 if n_pz % 2 == 0 and n_pz & (n_pz - 1) == 0 else 1
    half_rows = depth_y // halves
    for f in range(fields):
        for o in range(n_py - 1, 0, -1):
            copy_y(f, o).wait_recv()
        high, low = split(lines[f])
        for h in range(halves):
            part = lax.rem(pz // (n_pz // halves) + h + 1, halves)
            span = pl.ds(pl.multiple_of(part * half_rows, half_rows), half_rows)
            parts_out[f, span] = rows_transform(my[0, span], my[1, span], high, low)
            top = n_pz - h * (n_pz // halves)
            for o in range(top - 1, max(top - n_pz // halves, 1) - 1, -1):
                copy_z(f, o).start()
        parts[f, pl.ds(pz * rows_z, rows_z)] = parts_out[f, pl.ds(pz * rows_z, rows_z)]

    row, col = iota((rows_out, nz), 0), iota((rows_out, nz), 1)
    pick = (row % nz == col).astype(F32).astype(BF16)
    row, col = iota((nz, depth_z), 0), iota((nz, depth_z), 1)
    spread = ((col // rows_z) * zl + col % zl == row).astype(F32).astype(BF16)
    row, col = iota((rows_out, depth_z), 0), iota((rows_out, depth_z), 1)
    keep = row // nz == (col // zl) % share_y
    for t in range(2):
        wide = dot(dot(pick, hz[t]).astype(BF16), spread)
        mz[t] = jnp.where(keep, wide, 0.0).astype(BF16)

    diagonal = iota((nz, nz), 0) == iota((nz, nz), 1)
    sz_column = jnp.sum(jnp.where(diagonal, sz[...], 0.0), axis=1, keepdims=True)
    sx_row = sx[:, pl.ds(pl.multiple_of(py * share_x, share_x), share_x)]
    for k in range(share_y):
        symbol = (sx_row + sy[pz * share_y + k]) + sz_column
        weights[pl.ds(k * nz, nz)] = 1.0 / (1.0 + symbol)

    last = fields - 1
    for f in range(fields):
        for o in range(n_pz - 1, 0, -1):
            copy_z(f, o).wait_recv()
        high, low = split(parts[f])
        if f < last:
            modes[f] = rows_transform(mz[0], mz[1], high, low)
        if f == last - 1:
            for k in range(share_y):
                span = pl.ds(k * nz, nz)
                weight = weights[span]
                old = [modes[b, span] for b in range(last)]
                for a in range(fields):
                    mixed = coupling[a, 0] * old[0]
                    for b in range(1, last):
                        mixed = mixed + coupling[a, b] * old[b]
                    mixed = (1.0 - weight) * mixed
                    out_ref[a, span] = mixed + weight * old[a] if a < last else mixed
        if f == last:
            result = rows_transform(mz[0], mz[1], high, low)
            weight = weights[...]
            rest = (1.0 - weight) * result
            for a in range(fields):
                new = out_ref[a] + coupling[a, last] * rest
                out_ref[a] = new + weight * result if a == last else new
    for f in range(fields):
        for o in range(1, n_py):
            copy_y(f, o).wait_send()
        for o in range(1, n_pz):
            copy_z(f, o).wait_send()


def shards(n_py, n_pz, species, coupling, symbol_x, symbol_y, symbol_z):
    fields, nx, yl, zl = species.shape
    ny, nz = yl * n_py, zl * n_pz
    share_x, share_y = nx // n_py, ny // n_pz
    block = fields * nx * yl * zl
    tables = 2 * (nx * nx + (ny * zl) ** 2 + (share_y * nz) ** 2)
    need = 7 * 4 * block + 2 * tables + 16 * max(ny * zl, share_y * nz) ** 2
    if share_x % LANES or zl % SUBLANES or nx % n_py or ny % n_pz or need > VMEM_BUDGET or fields < 2:
        return plain_shards(species, coupling, symbol_x, symbol_y, symbol_z)
    dims = (fields, ny, nz, n_py, n_pz, yl, zl, share_x, share_y)
    rows_y, depth_y, depth_z = yl * zl, ny * zl, share_y * nz
    vmem = pl.BlockSpec(memory_space=pltpu.VMEM)
    hbm = pl.BlockSpec(memory_space=pltpu.HBM)
    values = jnp.transpose(species, (0, 2, 3, 1)).reshape(fields, rows_y, nx)
    out = pl.pallas_call(
        functools.partial(kernel, dims),
        out_shape=jax.ShapeDtypeStruct((fields, depth_z, share_x), F32),
        in_specs=[hbm] * 8,
        out_specs=vmem,
        scratch_shapes=[
            pltpu.VMEM((fields, rows_y, nx), F32),
            pltpu.VMEM((2, nx, nx), BF16),
            pltpu.VMEM((2, ny, ny), BF16),
            pltpu.VMEM((2, nz, nz), BF16),
            pltpu.SMEM((fields, fields), F32),
            pltpu.VMEM((1, nx), F32),
            pltpu.SMEM((ny,), F32),
            pltpu.VMEM((1, nz), F32),
            pltpu.VMEM((fields, n_py, rows_y, share_x), F32),
            pltpu.VMEM((fields, depth_y, share_x), F32),
            pltpu.VMEM((fields, depth_y, share_x), F32),
            pltpu.VMEM((fields, depth_z, share_x), F32),
            pltpu.VMEM((fields - 1, depth_z, share_x), F32),
            pltpu.VMEM((depth_z, share_x), F32),
            pltpu.VMEM((2, depth_y, depth_y), BF16),
            pltpu.VMEM((2, depth_z, depth_z), BF16),
            pltpu.SemaphoreType.DMA((fields,)),
            pltpu.SemaphoreType.DMA((8,)),
            pltpu.SemaphoreType.DMA((fields, n_py)),
            pltpu.SemaphoreType.DMA((fields, n_py)),
            pltpu.SemaphoreType.DMA((fields, n_pz)),
            pltpu.SemaphoreType.DMA((fields, n_pz)),
        ],
        compiler_params=pltpu.CompilerParams(
            collective_id=0, has_side_effects=True, vmem_limit_bytes=VMEM_BUDGET
        ),
    )(
        values,
        jnp.asarray(split_table(nx)),
        jnp.asarray(split_table(ny)),
        jnp.asarray(split_table(nz)),
        coupling,
        symbol_x.reshape(1, nx),
        symbol_y,
        symbol_z.reshape(1, nz),
    )
    return jnp.transpose(out.reshape(fields, share_y, nz, share_x), (0, 3, 1, 2))


def solution(mesh):
    return jax.shard_map(
        functools.partial(shards, mesh.shape["py"], mesh.shape["pz"]),
        mesh=mesh,
        in_specs=(P(None, None, "py", "pz"), P(), P(), P(), P()),
        out_specs=P(None, "py", "pz", None),
        check_vma=False,
    )
```

```python
import functools

import jax
import jax.numpy as jnp
import numpy as np
from jax import lax
from jax.experimental import pallas as pl
from jax.experimental.pallas import tpu as pltpu
from jax.sharding import PartitionSpec as P

MESH = pl.DeviceIdType.MESH
F32 = jnp.float32
BF16 = jnp.bfloat16
LANES, SUBLANES = 128, 8
VMEM_BUDGET = 48 << 20


def mode_table(count):
    rank = jnp.arange(count)
    angle = (
        jnp.pi
        / (4 * count)
        * ((2 * rank[:, None] + 1) * (2 * rank[None, :] + 1) % (8 * count)).astype(jnp.float32)
    )
    return jnp.cos(angle) * (2.0 / count) ** 0.5


def transform_dim(values, dim):
    moved = jnp.tensordot(
        values, mode_table(values.shape[dim]), axes=([dim], [0]), precision=lax.Precision.HIGHEST
    )
    return jnp.moveaxis(moved, -1, dim)


def plain_shards(species, coupling, symbol_x, symbol_y, symbol_z):
    values = transform_dim(species, 1)
    values = lax.all_to_all(values, "py", split_axis=1, concat_axis=2, tiled=True)
    values = transform_dim(values, 2)
    values = lax.all_to_all(values, "pz", split_axis=2, concat_axis=3, tiled=True)
    values = transform_dim(values, 3)
    share_x = values.shape[1]
    part_x = lax.dynamic_slice_in_dim(symbol_x, lax.axis_index("py") * share_x, share_x)
    share_y = values.shape[2]
    part_y = lax.dynamic_slice_in_dim(symbol_y, lax.axis_index("pz") * share_y, share_y)
    symbol = part_x[:, None, None] + part_y[None, :, None] + symbol_z[None, None, :]
    weight = 1.0 / (1.0 + symbol)
    mixed = jnp.einsum("ab,bxyz->axyz", coupling, values, precision=lax.Precision.HIGHEST)
    return weight * values + (1.0 - weight) * mixed


def split_table(count):
    rank = 2 * np.arange(count) + 1
    table = np.cos(np.pi / (4 * count) * (rank[:, None] * rank[None, :] % (8 * count)))
    table = (table * np.sqrt(2.0 / count)).astype(np.float32)
    high = table.astype(BF16)
    low = (table - high.astype(np.float32)).astype(BF16)
    return np.stack([high, low])


def split(values):
    high = values.astype(BF16)
    low = (values - high.astype(F32)).astype(BF16)
    return high, low


def dot(a, b):
    return jnp.dot(a, b, preferred_element_type=F32)


def flipped(index, offset, count):
    if count & (count - 1):
        return lax.rem(index + offset, count)
    result = index
    bit = 1
    while bit < count:
        if offset & bit:
            result = result + bit - 2 * bit * lax.rem(index // bit, 2)
        bit *= 2
    return result


def source_of(index, offset, count):
    if count & (count - 1):
        return lax.rem(index + count - offset, count)
    return flipped(index, offset, count)


def kernel(
    dims, field_ref, hx_hbm, hy_hbm, hz_hbm, coupling_hbm, sx_hbm, sy_hbm, sz_hbm, out_ref,
    held, hx, hy, hz, coupling, sx, sy, sz, lines_out, lines, parts_out, parts, modes, weights,
    my, mz, load_sem, side_sem, send_y, recv_y, send_z, recv_z,
):
    fields, ny, nz, n_py, n_pz, yl, zl, share_x, share_y = dims
    py, pz = lax.axis_index("py"), lax.axis_index("pz")
    rows_y = yl * zl
    rows_z = share_y * zl
    depth_y = ny * zl
    rows_out = share_y * nz
    depth_z = n_pz * rows_z

    def load(f):
        return pltpu.make_async_copy(field_ref.at[f], held.at[f], load_sem.at[f])

    pairs = (
        (hx_hbm.at[0], hx.at[0]), (hx_hbm.at[1], hx.at[1]), (hy_hbm, hy), (hz_hbm, hz),
        (coupling_hbm, coupling), (sx_hbm, sx), (sy_hbm, sy), (sz_hbm, sz),
    )
    sides = [
        pltpu.make_async_copy(a, b, side_sem.at[i]) for i, (a, b) in enumerate(pairs)
    ]
    load(0).start()
    sides[0].start()
    sides[1].start()
    for f in range(1, fields):
        load(f).start()
    for side in sides[2:]:
        side.start()
    barrier = pltpu.get_barrier_semaphore()
    for o in range(1, n_pz):
        pl.semaphore_signal(
            barrier, inc=1, device_id={"pz": flipped(pz, o, n_pz)}, device_id_type=MESH
        )
    for o in range(1, n_py):
        pl.semaphore_signal(
            barrier, inc=1, device_id={"py": flipped(py, o, n_py)}, device_id_type=MESH
        )

    def copy_y(f, o):
        to = flipped(py, o, n_py)
        return pltpu.make_async_remote_copy(
            src_ref=lines_out.at[f, to],
            dst_ref=lines.at[f, pl.ds(py * rows_y, rows_y)],
            send_sem=send_y.at[f, o],
            recv_sem=recv_y.at[f, o],
            device_id={"py": to},
            device_id_type=MESH,
        )

    def copy_z(f, o):
        to = flipped(pz, o, n_pz)
        return pltpu.make_async_remote_copy(
            src_ref=parts_out.at[f, pl.ds(to * rows_z, rows_z)],
            dst_ref=parts.at[f, pl.ds(pz * rows_z, rows_z)],
            send_sem=send_z.at[f, o],
            recv_sem=recv_z.at[f, o],
            device_id={"pz": to},
            device_id_type=MESH,
        )

    for f in range(fields):
        load(f).wait()
        high, low = split(held[f])
        if f == 0:
            sides[0].wait()
            sides[1].wait()
        both = dot(jnp.concatenate([high, low], axis=0), hx[0])
        result = both[:rows_y] + both[rows_y:] + dot(high, hx[1])
        for d in range(n_py):
            lines_out[f, d] = result[:, d * share_x : (d + 1) * share_x]
        if f == 0:
            pl.semaphore_wait(barrier, n_py + n_pz - 2)
        for o in range(n_py - 1, 0, -1):
            copy_y(f, o).start()
        lines[f, pl.ds(py * rows_y, rows_y)] = lines_out[f, py]

    for side in sides[2:]:
        side.wait()

    def iota(shape, dim):
        return lax.broadcasted_iota(jnp.int32, shape, dim)

    row, col = iota((depth_y, ny), 0), iota((depth_y, ny), 1)
    pick = (row // zl == col).astype(F32).astype(BF16)
    row, col = iota((ny, depth_y), 0), iota((ny, depth_y), 1)
    spread = (col // zl == row).astype(F32).astype(BF16)
    row, col = iota((depth_y, depth_y), 0), iota((depth_y, depth_y), 1)
    keep = row % zl == col % zl
    for t in range(2):
        wide = dot(dot(pick, hy[t]).astype(BF16), spread)
        my[t] = jnp.where(keep, wide, 0.0).astype(BF16)
    def rows_transform(high_table, low_table, high, low):
        both = dot(high_table, jnp.concatenate([high, low], axis=1))
        return both[:, :share_x] + both[:, share_x:] + dot(low_table, high)

    halves = 2 if n_pz % 2 == 0 and n_pz & (n_pz - 1) == 0 else 1
    half_rows = depth_y // halves
    for f in range(fields):
        for o in range(n_py - 1, 0, -1):
            copy_y(f, o).wait_recv()
        high, low = split(lines[f])
        for h in range(halves):
            part = lax.rem(pz // (n_pz // halves) + h + 1, halves)
            span = pl.ds(pl.multiple_of(part * half_rows, half_rows), half_rows)
            parts_out[f, span] = rows_transform(my[0, span], my[1, span], high, low)
            top = n_pz - h * (n_pz // halves)
            for o in range(top - 1, max(top - n_pz // halves, 1) - 1, -1):
                copy_z(f, o).start()
        parts[f, pl.ds(pz * rows_z, rows_z)] = parts_out[f, pl.ds(pz * rows_z, rows_z)]

    row, col = iota((rows_out, nz), 0), iota((rows_out, nz), 1)
    pick = (row % nz == col).astype(F32).astype(BF16)
    row, col = iota((nz, depth_z), 0), iota((nz, depth_z), 1)
    spread = ((col // rows_z) * zl + col % zl == row).astype(F32).astype(BF16)
    row, col = iota((rows_out, depth_z), 0), iota((rows_out, depth_z), 1)
    keep = row // nz == (col // zl) % share_y
    for t in range(2):
        wide = dot(dot(pick, hz[t]).astype(BF16), spread)
        mz[t] = jnp.where(keep, wide, 0.0).astype(BF16)

    diagonal = iota((nz, nz), 0) == iota((nz, nz), 1)
    sz_column = jnp.sum(jnp.where(diagonal, sz[...], 0.0), axis=1, keepdims=True)
    sx_row = sx[:, pl.ds(pl.multiple_of(py * share_x, share_x), share_x)]
    for k in range(share_y):
        symbol = (sx_row + sy[pz * share_y + k]) + sz_column
        weights[pl.ds(k * nz, nz)] = 1.0 / (1.0 + symbol)

    last = fields - 1
    for f in range(fields):
        for o in range(n_pz - 1, 0, -1):
            copy_z(f, o).wait_recv()
        high, low = split(parts[f])
        if f < last:
            modes[f] = rows_transform(mz[0], mz[1], high, low)
        if f == last - 1:
            for k in range(share_y):
                span = pl.ds(k * nz, nz)
                weight = weights[span]
                old = [modes[b, span] for b in range(last)]
                for a in range(fields):
                    mixed = coupling[a, 0] * old[0]
                    for b in range(1, last):
                        mixed = mixed + coupling[a, b] * old[b]
                    mixed = (1.0 - weight) * mixed
                    out_ref[a, span] = mixed + weight * old[a] if a < last else mixed
        if f == last:
            result = rows_transform(mz[0], mz[1], high, low)
            weight = weights[...]
            rest = (1.0 - weight) * result
            for a in range(fields):
                new = out_ref[a] + coupling[a, last] * rest
                out_ref[a] = new + weight * result if a == last else new
    for f in range(fields):
        for o in range(1, n_py):
            copy_y(f, o).wait_send()
        for o in range(1, n_pz):
            copy_z(f, o).wait_send()


def shards(n_py, n_pz, species, coupling, symbol_x, symbol_y, symbol_z):
    fields, nx, yl, zl = species.shape
    ny, nz = yl * n_py, zl * n_pz
    share_x, share_y = nx // n_py, ny // n_pz
    block = fields * nx * yl * zl
    tables = 2 * (nx * nx + (ny * zl) ** 2 + (share_y * nz) ** 2)
    need = 7 * 4 * block + 2 * tables + 16 * max(ny * zl, share_y * nz) ** 2
    if share_x % LANES or zl % SUBLANES or nx % n_py or ny % n_pz or need > VMEM_BUDGET or fields < 2:
        return plain_shards(species, coupling, symbol_x, symbol_y, symbol_z)
    dims = (fields, ny, nz, n_py, n_pz, yl, zl, share_x, share_y)
    rows_y, depth_y, depth_z = yl * zl, ny * zl, share_y * nz
    vmem = pl.BlockSpec(memory_space=pltpu.VMEM)
    hbm = pl.BlockSpec(memory_space=pltpu.HBM)
    values = jnp.transpose(species, (0, 2, 3, 1)).reshape(fields, rows_y, nx)
    out = pl.pallas_call(
        functools.partial(kernel, dims),
        out_shape=jax.ShapeDtypeStruct((fields, depth_z, share_x), F32),
        in_specs=[hbm] * 8,
        out_specs=vmem,
        scratch_shapes=[
            pltpu.VMEM((fields, rows_y, nx), F32),
            pltpu.VMEM((2, nx, nx), BF16),
            pltpu.VMEM((2, ny, ny), BF16),
            pltpu.VMEM((2, nz, nz), BF16),
            pltpu.SMEM((fields, fields), F32),
            pltpu.VMEM((1, nx), F32),
            pltpu.SMEM((ny,), F32),
            pltpu.VMEM((1, nz), F32),
            pltpu.VMEM((fields, n_py, rows_y, share_x), F32),
            pltpu.VMEM((fields, depth_y, share_x), F32),
            pltpu.VMEM((fields, depth_y, share_x), F32),
            pltpu.VMEM((fields, depth_z, share_x), F32),
            pltpu.VMEM((fields - 1, depth_z, share_x), F32),
            pltpu.VMEM((depth_z, share_x), F32),
            pltpu.VMEM((2, depth_y, depth_y), BF16),
            pltpu.VMEM((2, depth_z, depth_z), BF16),
            pltpu.SemaphoreType.DMA((fields,)),
            pltpu.SemaphoreType.DMA((8,)),
            pltpu.SemaphoreType.DMA((fields, n_py)),
            pltpu.SemaphoreType.DMA((fields, n_py)),
            pltpu.SemaphoreType.DMA((fields, n_pz)),
            pltpu.SemaphoreType.DMA((fields, n_pz)),
        ],
        compiler_params=pltpu.CompilerParams(
            collective_id=0, has_side_effects=True, vmem_limit_bytes=67043328
        ),
    )(
        values,
        jnp.asarray(split_table(nx)),
        jnp.asarray(split_table(ny)),
        jnp.asarray(split_table(nz)),
        coupling,
        symbol_x.reshape(1, nx),
        symbol_y,
        symbol_z.reshape(1, nz),
    )
    return jnp.transpose(out.reshape(fields, share_y, nz, share_x), (0, 3, 1, 2))


def solution(mesh):
    return jax.shard_map(
        functools.partial(shards, mesh.shape["py"], mesh.shape["pz"]),
        mesh=mesh,
        in_specs=(P(None, None, "py", "pz"), P(), P(), P(), P()),
        out_specs=P(None, "py", "pz", None),
        check_vma=False,
    )
```

```python
import functools

import jax
import jax.numpy as jnp
import numpy as np
from jax import lax
from jax.experimental import pallas as pl
from jax.experimental.pallas import tpu as pltpu
from jax.sharding import PartitionSpec as P

MESH = pl.DeviceIdType.MESH
F32 = jnp.float32
BF16 = jnp.bfloat16
LANES, SUBLANES = 128, 8
CUTS = 2
VMEM_BUDGET = 48 << 20


def mode_table(count):
    rank = jnp.arange(count)
    angle = (
        jnp.pi
        / (4 * count)
        * ((2 * rank[:, None] + 1) * (2 * rank[None, :] + 1) % (8 * count)).astype(jnp.float32)
    )
    return jnp.cos(angle) * (2.0 / count) ** 0.5


def transform_dim(values, dim):
    moved = jnp.tensordot(
        values, mode_table(values.shape[dim]), axes=([dim], [0]), precision=lax.Precision.HIGHEST
    )
    return jnp.moveaxis(moved, -1, dim)


def plain_shards(species, coupling, symbol_x, symbol_y, symbol_z):
    values = transform_dim(species, 1)
    values = lax.all_to_all(values, "py", split_axis=1, concat_axis=2, tiled=True)
    values = transform_dim(values, 2)
    values = lax.all_to_all(values, "pz", split_axis=2, concat_axis=3, tiled=True)
    values = transform_dim(values, 3)
    share_x = values.shape[1]
    part_x = lax.dynamic_slice_in_dim(symbol_x, lax.axis_index("py") * share_x, share_x)
    share_y = values.shape[2]
    part_y = lax.dynamic_slice_in_dim(symbol_y, lax.axis_index("pz") * share_y, share_y)
    symbol = part_x[:, None, None] + part_y[None, :, None] + symbol_z[None, None, :]
    weight = 1.0 / (1.0 + symbol)
    mixed = jnp.einsum("ab,bxyz->axyz", coupling, values, precision=lax.Precision.HIGHEST)
    return weight * values + (1.0 - weight) * mixed


def split_table(count):
    rank = 2 * np.arange(count) + 1
    table = np.cos(np.pi / (4 * count) * (rank[:, None] * rank[None, :] % (8 * count)))
    table = (table * np.sqrt(2.0 / count)).astype(np.float32)
    high = table.astype(BF16)
    low = (table - high.astype(np.float32)).astype(BF16)
    return np.stack([high, low])


def split(values):
    high = values.astype(BF16)
    low = (values - high.astype(F32)).astype(BF16)
    return high, low


def dot(a, b):
    return jnp.dot(a, b, preferred_element_type=F32)


def flipped(index, offset, count):
    if count & (count - 1):
        return lax.rem(index + offset, count)
    result = index
    bit = 1
    while bit < count:
        if offset & bit:
            result = result + bit - 2 * bit * lax.rem(index // bit, 2)
        bit *= 2
    return result


def source_of(index, offset, count):
    if count & (count - 1):
        return lax.rem(index + count - offset, count)
    return flipped(index, offset, count)


def kernel(
    dims, field_ref, hx_hbm, hy_hbm, hz_hbm, coupling_hbm, sx_hbm, sy_hbm, sz_hbm, out_ref,
    held, hx, hy, hz, coupling, sx, sy, sz, lines_out, lines, parts_out, parts, modes, weights,
    my, mz, load_sem, side_sem, send_y, recv_y, send_z, recv_z,
):
    fields, ny, nz, n_py, n_pz, yl, zl, share_x, share_y = dims
    py, pz = lax.axis_index("py"), lax.axis_index("pz")
    zc = zl // CUTS
    rows_y = yl * zc
    rows_z = share_y * zc
    depth_y = ny * zc
    rows_out = share_y * nz
    depth_z = n_pz * rows_z * CUTS

    columns = field_ref.shape[2] // LANES

    def load(f):
        return [
            pltpu.make_async_copy(
                field_ref.at[f, :, pl.ds(j * LANES, LANES)], held.at[f, j], load_sem.at[f, j]
            )
            for j in range(columns)
        ]

    pairs = (
        (hx_hbm.at[0], hx.at[0]), (hx_hbm.at[1], hx.at[1]), (hy_hbm, hy), (hz_hbm, hz),
        (coupling_hbm, coupling), (sx_hbm, sx), (sy_hbm, sy), (sz_hbm, sz),
    )
    sides = [
        pltpu.make_async_copy(a, b, side_sem.at[i]) for i, (a, b) in enumerate(pairs)
    ]
    for part in load(0):
        part.start()
    sides[0].start()
    sides[1].start()
    for f in range(1, fields):
        for part in load(f):
            part.start()
    for side in sides[2:]:
        side.start()
    barrier = pltpu.get_barrier_semaphore()
    for o in range(1, n_pz):
        pl.semaphore_signal(
            barrier, inc=1, device_id={"pz": flipped(pz, o, n_pz)}, device_id_type=MESH
        )
    for o in range(1, n_py):
        pl.semaphore_signal(
            barrier, inc=1, device_id={"py": flipped(py, o, n_py)}, device_id_type=MESH
        )

    def copy_y(f, c, o):
        to = flipped(py, o, n_py)
        return pltpu.make_async_remote_copy(
            src_ref=lines_out.at[f, c, to],
            dst_ref=lines.at[f, c, pl.ds(py * rows_y, rows_y)],
            send_sem=send_y.at[f * CUTS + c, o],
            recv_sem=recv_y.at[f * CUTS + c, o],
            device_id={"py": to},
            device_id_type=MESH,
        )

    def copy_z(f, c, o):
        to = flipped(pz, o, n_pz)
        return pltpu.make_async_remote_copy(
            src_ref=parts_out.at[f, c, pl.ds(to * rows_z, rows_z)],
            dst_ref=parts.at[f, pl.ds((pz * CUTS + c) * rows_z, rows_z)],
            send_sem=send_z.at[f * CUTS + c, o],
            recv_sem=recv_z.at[f * CUTS + c, o],
            device_id={"pz": to},
            device_id_type=MESH,
        )

    for f in range(fields):
        for part in load(f):
            part.wait()
        batches = [[c] for c in range(CUTS)] if f == 0 else [list(range(CUTS))]
        for batch in batches:
            span = range(batch[0] * zc, (batch[-1] + 1) * zc)
            blocks = [
                jnp.concatenate([held[f, j, pl.ds(z, yl, stride=zl)] for z in span], axis=0)
                for j in range(columns)
            ]
            high, low = split(jnp.concatenate(blocks, axis=1))
            count = len(batch) * rows_y
            if f == 0 and batch[0] == 0:
                sides[0].wait()
                sides[1].wait()
            both = dot(jnp.concatenate([high, low], axis=0), hx[0])
            result = both[:count] + both[count:] + dot(high, hx[1])
            for i, c in enumerate(batch):
                for d in range(n_py):
                    lines_out[f, c, d] = result[
                        i * rows_y : (i + 1) * rows_y, d * share_x : (d + 1) * share_x
                    ]
            if f == 0 and batch[0] == 0:
                pl.semaphore_wait(barrier, n_py + n_pz - 2)
            for c in batch:
                for o in range(n_py - 1, 0, -1):
                    copy_y(f, c, o).start()
                lines[f, c, pl.ds(py * rows_y, rows_y)] = lines_out[f, c, py]

    for side in sides[2:]:
        side.wait()

    def iota(shape, dim):
        return lax.broadcasted_iota(jnp.int32, shape, dim)

    row, col = iota((depth_y, ny), 0), iota((depth_y, ny), 1)
    pick = (row // zc == col).astype(F32).astype(BF16)
    row, col = iota((ny, depth_y), 0), iota((ny, depth_y), 1)
    spread = ((col // rows_y) * yl + col % yl == row).astype(F32).astype(BF16)
    row, col = iota((depth_y, depth_y), 0), iota((depth_y, depth_y), 1)
    keep = row % zc == (col // yl) % zc
    for t in range(2):
        wide = dot(dot(pick, hy[t]).astype(BF16), spread)
        my[t] = jnp.where(keep, wide, 0.0).astype(BF16)
    def rows_transform(high_table, low_table, high, low):
        both = dot(high_table, jnp.concatenate([high, low], axis=1))
        return both[:, :share_x] + both[:, share_x:] + dot(low_table, high)

    halves = 2 if n_pz % 2 == 0 and n_pz & (n_pz - 1) == 0 else 1
    half_rows = depth_y // halves
    for f, c in [(f, c) for f in range(fields) for c in range(CUTS)]:
        for o in range(n_py - 1, 0, -1):
            copy_y(f, c, o).wait_recv()
        high, low = split(lines[f, c])
        for h in range(halves):
            part = lax.rem(pz // (n_pz // halves) + h + 1, halves)
            span = pl.ds(pl.multiple_of(part * half_rows, half_rows), half_rows)
            parts_out[f, c, span] = rows_transform(my[0, span], my[1, span], high, low)
            top = n_pz - h * (n_pz // halves)
            for o in range(top - 1, max(top - n_pz // halves, 1) - 1, -1):
                copy_z(f, c, o).start()
        parts[f, pl.ds((pz * CUTS + c) * rows_z, rows_z)] = parts_out[
            f, c, pl.ds(pz * rows_z, rows_z)
        ]

    row, col = iota((rows_out, nz), 0), iota((rows_out, nz), 1)
    pick = (row % nz == col).astype(F32).astype(BF16)
    row, col = iota((nz, depth_z), 0), iota((nz, depth_z), 1)
    spread = ((col // rows_z) * zc + col % zc == row).astype(F32).astype(BF16)
    row, col = iota((rows_out, depth_z), 0), iota((rows_out, depth_z), 1)
    keep = row // nz == (col // zc) % share_y
    for t in range(2):
        wide = dot(dot(pick, hz[t]).astype(BF16), spread)
        mz[t] = jnp.where(keep, wide, 0.0).astype(BF16)

    diagonal = iota((nz, nz), 0) == iota((nz, nz), 1)
    sz_column = jnp.sum(jnp.where(diagonal, sz[...], 0.0), axis=1, keepdims=True)
    sx_row = sx[:, pl.ds(pl.multiple_of(py * share_x, share_x), share_x)]
    for k in range(share_y):
        symbol = (sx_row + sy[pz * share_y + k]) + sz_column
        weights[pl.ds(k * nz, nz)] = 1.0 / (1.0 + symbol)

    last = fields - 1
    for f in range(fields):
        for c in range(CUTS):
            for o in range(n_pz - 1, 0, -1):
                copy_z(f, c, o).wait_recv()
        high, low = split(parts[f])
        if f < last:
            modes[f] = rows_transform(mz[0], mz[1], high, low)
        if f == last - 1:
            for k in range(share_y):
                span = pl.ds(k * nz, nz)
                weight = weights[span]
                old = [modes[b, span] for b in range(last)]
                for a in range(fields):
                    mixed = coupling[a, 0] * old[0]
                    for b in range(1, last):
                        mixed = mixed + coupling[a, b] * old[b]
                    mixed = (1.0 - weight) * mixed
                    out_ref[a, span] = mixed + weight * old[a] if a < last else mixed
        if f == last:
            result = rows_transform(mz[0], mz[1], high, low)
            weight = weights[...]
            rest = (1.0 - weight) * result
            for a in range(fields):
                new = out_ref[a] + coupling[a, last] * rest
                out_ref[a] = new + weight * result if a == last else new
    for f, c in [(f, c) for f in range(fields) for c in range(CUTS)]:
        for o in range(1, n_py):
            copy_y(f, c, o).wait_send()
        for o in range(1, n_pz):
            copy_z(f, c, o).wait_send()


def shards(n_py, n_pz, species, coupling, symbol_x, symbol_y, symbol_z):
    fields, nx, yl, zl = species.shape
    ny, nz = yl * n_py, zl * n_pz
    share_x, share_y = nx // n_py, ny // n_pz
    block = fields * nx * yl * zl
    tables = 2 * (nx * nx + (ny * zl) ** 2 + (share_y * nz) ** 2)
    need = 7 * 4 * block + 2 * tables + 16 * max(ny * zl, share_y * nz) ** 2
    fits = need <= VMEM_BUDGET and fields > 1 and zl % CUTS == 0 and nz % SUBLANES == 0
    fits = fits and yl % SUBLANES == 0 and share_y * (zl // CUTS) % SUBLANES == 0
    if share_x % LANES or nx % n_py or ny % n_pz or not fits:
        return plain_shards(species, coupling, symbol_x, symbol_y, symbol_z)
    dims = (fields, ny, nz, n_py, n_pz, yl, zl, share_x, share_y)
    rows_y, depth_y, depth_z = yl * zl // CUTS, ny * zl // CUTS, share_y * nz
    vmem = pl.BlockSpec(memory_space=pltpu.VMEM)
    hbm = pl.BlockSpec(memory_space=pltpu.HBM)
    values = jnp.transpose(species, (0, 2, 3, 1)).reshape(fields, yl * zl, nx)
    out = pl.pallas_call(
        functools.partial(kernel, dims),
        out_shape=jax.ShapeDtypeStruct((fields, depth_z, share_x), F32),
        in_specs=[hbm] * 8,
        out_specs=vmem,
        scratch_shapes=[
            pltpu.VMEM((fields, nx // LANES, yl * zl, LANES), F32),
            pltpu.VMEM((2, nx, nx), BF16),
            pltpu.VMEM((2, ny, ny), BF16),
            pltpu.VMEM((2, nz, nz), BF16),
            pltpu.SMEM((fields, fields), F32),
            pltpu.VMEM((1, nx), F32),
            pltpu.SMEM((ny,), F32),
            pltpu.VMEM((1, nz), F32),
            pltpu.VMEM((fields, CUTS, n_py, rows_y, share_x), F32),
            pltpu.VMEM((fields, CUTS, depth_y, share_x), F32),
            pltpu.VMEM((fields, CUTS, depth_y, share_x), F32),
            pltpu.VMEM((fields, depth_z, share_x), F32),
            pltpu.VMEM((fields - 1, depth_z, share_x), F32),
            pltpu.VMEM((depth_z, share_x), F32),
            pltpu.VMEM((2, depth_y, depth_y), BF16),
            pltpu.VMEM((2, depth_z, depth_z), BF16),
            pltpu.SemaphoreType.DMA((fields, nx // LANES)),
            pltpu.SemaphoreType.DMA((8,)),
            pltpu.SemaphoreType.DMA((fields * CUTS, n_py)),
            pltpu.SemaphoreType.DMA((fields * CUTS, n_py)),
            pltpu.SemaphoreType.DMA((fields * CUTS, n_pz)),
            pltpu.SemaphoreType.DMA((fields * CUTS, n_pz)),
        ],
        compiler_params=pltpu.CompilerParams(
            collective_id=0, has_side_effects=True, vmem_limit_bytes=67043328
        ),
    )(
        values,
        jnp.asarray(split_table(nx)),
        jnp.asarray(split_table(ny)),
        jnp.asarray(split_table(nz)),
        coupling,
        symbol_x.reshape(1, nx),
        symbol_y,
        symbol_z.reshape(1, nz),
    )
    return jnp.transpose(out.reshape(fields, share_y, nz, share_x), (0, 3, 1, 2))


def solution(mesh):
    return jax.shard_map(
        functools.partial(shards, mesh.shape["py"], mesh.shape["pz"]),
        mesh=mesh,
        in_specs=(P(None, None, "py", "pz"), P(), P(), P(), P()),
        out_specs=P(None, "py", "pz", None),
        check_vma=False,
    )
```

```python
import functools

import jax
import jax.numpy as jnp
import numpy as np
from jax import lax
from jax.experimental import pallas as pl
from jax.experimental.pallas import tpu as pltpu
from jax.sharding import PartitionSpec as P

MESH = pl.DeviceIdType.MESH
F32 = jnp.float32
BF16 = jnp.bfloat16
LANES, SUBLANES = 128, 8
VMEM_BUDGET = 48 << 20


def mode_table(count):
    rank = jnp.arange(count)
    angle = (
        jnp.pi
        / (4 * count)
        * ((2 * rank[:, None] + 1) * (2 * rank[None, :] + 1) % (8 * count)).astype(jnp.float32)
    )
    return jnp.cos(angle) * (2.0 / count) ** 0.5


def transform_dim(values, dim):
    moved = jnp.tensordot(
        values, mode_table(values.shape[dim]), axes=([dim], [0]), precision=lax.Precision.HIGHEST
    )
    return jnp.moveaxis(moved, -1, dim)


def plain_shards(species, coupling, symbol_x, symbol_y, symbol_z):
    values = transform_dim(species, 1)
    values = lax.all_to_all(values, "py", split_axis=1, concat_axis=2, tiled=True)
    values = transform_dim(values, 2)
    values = lax.all_to_all(values, "pz", split_axis=2, concat_axis=3, tiled=True)
    values = transform_dim(values, 3)
    share_x = values.shape[1]
    part_x = lax.dynamic_slice_in_dim(symbol_x, lax.axis_index("py") * share_x, share_x)
    share_y = values.shape[2]
    part_y = lax.dynamic_slice_in_dim(symbol_y, lax.axis_index("pz") * share_y, share_y)
    symbol = part_x[:, None, None] + part_y[None, :, None] + symbol_z[None, None, :]
    weight = 1.0 / (1.0 + symbol)
    mixed = jnp.einsum("ab,bxyz->axyz", coupling, values, precision=lax.Precision.HIGHEST)
    return weight * values + (1.0 - weight) * mixed


def split_table(count):
    rank = 2 * np.arange(count) + 1
    table = np.cos(np.pi / (4 * count) * (rank[:, None] * rank[None, :] % (8 * count)))
    table = (table * np.sqrt(2.0 / count)).astype(np.float32)
    high = table.astype(BF16)
    low = (table - high.astype(np.float32)).astype(BF16)
    return np.stack([high, low])


def split(values):
    high = values.astype(BF16)
    low = (values - high.astype(F32)).astype(BF16)
    return high, low


def dot(a, b):
    return jnp.dot(a, b, preferred_element_type=F32)


def flipped(index, offset, count):
    if count & (count - 1):
        return lax.rem(index + offset, count)
    result = index
    bit = 1
    while bit < count:
        if offset & bit:
            result = result + bit - 2 * bit * lax.rem(index // bit, 2)
        bit *= 2
    return result


def source_of(index, offset, count):
    if count & (count - 1):
        return lax.rem(index + count - offset, count)
    return flipped(index, offset, count)


def kernel(
    dims, field_ref, hx_hbm, hy_hbm, hz_hbm, coupling_hbm, sx_hbm, sy_hbm, sz_hbm, out_ref,
    held, hx, hy, hz, coupling, sx, sy, sz, lines_out, lines, parts_out, parts, modes, weights,
    my, mz, load_sem, side_sem, send_y, recv_y, send_z, recv_z,
):
    fields, ny, nz, n_py, n_pz, yl, zl, share_x, share_y = dims
    py, pz = lax.axis_index("py"), lax.axis_index("pz")
    rows_y = yl * zl
    rows_z = share_y * zl
    depth_y = ny * zl
    rows_out = share_y * nz
    depth_z = n_pz * rows_z

    def load(f):
        return pltpu.make_async_copy(field_ref.at[f], held.at[f], load_sem.at[f])

    pairs = (
        (hx_hbm.at[0], hx.at[0]), (hx_hbm.at[1], hx.at[1]), (hy_hbm, hy), (hz_hbm, hz),
        (coupling_hbm, coupling), (sx_hbm, sx), (sy_hbm, sy), (sz_hbm, sz),
    )
    sides = [
        pltpu.make_async_copy(a, b, side_sem.at[i]) for i, (a, b) in enumerate(pairs)
    ]
    load(0).start()
    sides[0].start()
    sides[1].start()
    for f in range(1, fields):
        load(f).start()
    for side in sides[2:]:
        side.start()
    barrier = pltpu.get_barrier_semaphore()
    for o in range(1, n_pz):
        pl.semaphore_signal(
            barrier, inc=1, device_id={"pz": flipped(pz, o, n_pz)}, device_id_type=MESH
        )
    for o in range(1, n_py):
        pl.semaphore_signal(
            barrier, inc=1, device_id={"py": flipped(py, o, n_py)}, device_id_type=MESH
        )

    def copy_y(f, o):
        to = flipped(py, o, n_py)
        return pltpu.make_async_remote_copy(
            src_ref=lines_out.at[f, to],
            dst_ref=lines.at[f, pl.ds(py * rows_y, rows_y)],
            send_sem=send_y.at[f, o],
            recv_sem=recv_y.at[f, o],
            device_id={"py": to},
            device_id_type=MESH,
        )

    def copy_z(f, o):
        to = flipped(pz, o, n_pz)
        return pltpu.make_async_remote_copy(
            src_ref=parts_out.at[f, pl.ds(to * rows_z, rows_z)],
            dst_ref=parts.at[f, pl.ds(pz * rows_z, rows_z)],
            send_sem=send_z.at[f, o],
            recv_sem=recv_z.at[f, o],
            device_id={"pz": to},
            device_id_type=MESH,
        )

    for f in range(fields):
        load(f).wait()
        high, low = split(held[f])
        if f == 0:
            sides[0].wait()
            sides[1].wait()
        both = dot(jnp.concatenate([high, low], axis=0), hx[0])
        result = both[:rows_y] + both[rows_y:] + dot(high, hx[1])
        for d in range(n_py):
            lines_out[f, d] = result[:, d * share_x : (d + 1) * share_x]
        if f == 0:
            pl.semaphore_wait(barrier, n_py + n_pz - 2)
        for o in range(n_py - 1, 0, -1):
            copy_y(f, o).start()
        lines[f, pl.ds(py * rows_y, rows_y)] = lines_out[f, py]

    for side in sides[2:]:
        side.wait()

    def iota(shape, dim):
        return lax.broadcasted_iota(jnp.int32, shape, dim)

    row, col = iota((depth_y, ny), 0), iota((depth_y, ny), 1)
    pick = (row // zl == col).astype(F32).astype(BF16)
    row, col = iota((ny, depth_y), 0), iota((ny, depth_y), 1)
    spread = (col // zl == row).astype(F32).astype(BF16)
    row, col = iota((depth_y, depth_y), 0), iota((depth_y, depth_y), 1)
    keep = row % zl == col % zl
    for t in range(2):
        wide = dot(dot(pick, hy[t]).astype(BF16), spread)
        my[t] = jnp.where(keep, wide, 0.0).astype(BF16)
    def rows_transform(high_table, low_table, high, low):
        both = dot(high_table, jnp.concatenate([high, low], axis=1))
        return both[:, :share_x] + both[:, share_x:] + dot(low_table, high)

    halves = 2 if n_pz % 2 == 0 and n_pz & (n_pz - 1) == 0 else 1
    half_rows = depth_y // halves
    for f in range(fields):
        for o in range(n_py - 1, 0, -1):
            copy_y(f, o).wait_recv()
        high, low = split(lines[f])
        for h in range(halves):
            part = lax.rem(pz // (n_pz // halves) + h + 1, halves)
            span = pl.ds(pl.multiple_of(part * half_rows, half_rows), half_rows)
            parts_out[f, span] = rows_transform(my[0, span], my[1, span], high, low)
            top = n_pz - h * (n_pz // halves)
            for o in range(top - 1, max(top - n_pz // halves, 1) - 1, -1):
                copy_z(f, o).start()
        parts[f, pl.ds(pz * rows_z, rows_z)] = parts_out[f, pl.ds(pz * rows_z, rows_z)]

    row, col = iota((rows_out, nz), 0), iota((rows_out, nz), 1)
    pick = (row % nz == col).astype(F32).astype(BF16)
    row, col = iota((nz, depth_z), 0), iota((nz, depth_z), 1)
    spread = ((col // rows_z) * zl + col % zl == row).astype(F32).astype(BF16)
    row, col = iota((rows_out, depth_z), 0), iota((rows_out, depth_z), 1)
    keep = row // nz == (col // zl) % share_y
    for t in range(2):
        wide = dot(dot(pick, hz[t]).astype(BF16), spread)
        mz[t] = jnp.where(keep, wide, 0.0).astype(BF16)

    diagonal = iota((nz, nz), 0) == iota((nz, nz), 1)
    sz_column = jnp.sum(jnp.where(diagonal, sz[...], 0.0), axis=1, keepdims=True)
    sx_row = sx[:, pl.ds(pl.multiple_of(py * share_x, share_x), share_x)]
    for k in range(share_y):
        symbol = (sx_row + sy[pz * share_y + k]) + sz_column
        weights[pl.ds(k * nz, nz)] = 1.0 / (1.0 + symbol)

    last = fields - 1
    for f in range(fields):
        for o in range(n_pz - 1, 0, -1):
            copy_z(f, o).wait_recv()
        high, low = split(parts[f])
        if f < last:
            modes[f] = rows_transform(mz[0], mz[1], high, low)
        if f == last - 1:
            for k in range(share_y):
                span = pl.ds(k * nz, nz)
                weight = weights[span]
                old = [modes[b, span] for b in range(last)]
                for a in range(fields):
                    mixed = coupling[a, 0] * old[0]
                    for b in range(1, last):
                        mixed = mixed + coupling[a, b] * old[b]
                    mixed = (1.0 - weight) * mixed
                    out_ref[a, span] = mixed + weight * old[a] if a < last else mixed
        if f == last:
            result = rows_transform(mz[0], mz[1], high, low)
            weight = weights[...]
            rest = (1.0 - weight) * result
            for a in range(fields):
                new = out_ref[a] + coupling[a, last] * rest
                out_ref[a] = new + weight * result if a == last else new
    for f in range(fields):
        for o in range(1, n_py):
            copy_y(f, o).wait_send()
        for o in range(1, n_pz):
            copy_z(f, o).wait_send()


def shards(n_py, n_pz, species, coupling, symbol_x, symbol_y, symbol_z):
    fields, nx, yl, zl = species.shape
    ny, nz = yl * n_py, zl * n_pz
    share_x, share_y = nx // n_py, ny // n_pz
    block = fields * nx * yl * zl
    tables = 2 * (nx * nx + (ny * zl) ** 2 + (share_y * nz) ** 2)
    need = 7 * 4 * block + 2 * tables + 16 * max(ny * zl, share_y * nz) ** 2
    if share_x % LANES or zl % SUBLANES or nx % n_py or ny % n_pz or need > VMEM_BUDGET or fields < 2:
        return plain_shards(species, coupling, symbol_x, symbol_y, symbol_z)
    dims = (fields, ny, nz, n_py, n_pz, yl, zl, share_x, share_y)
    rows_y, depth_y, depth_z = yl * zl, ny * zl, share_y * nz
    vmem = pl.BlockSpec(memory_space=pltpu.VMEM)
    hbm = pl.BlockSpec(memory_space=pltpu.HBM)
    values = jnp.transpose(species, (0, 2, 3, 1)).reshape(fields, rows_y, nx)
    out = pl.pallas_call(
        functools.partial(kernel, dims),
        out_shape=jax.ShapeDtypeStruct((fields, depth_z, share_x), F32),
        in_specs=[hbm] * 8,
        out_specs=vmem,
        scratch_shapes=[
            pltpu.VMEM((fields, rows_y, nx), F32),
            pltpu.VMEM((2, nx, nx), BF16),
            pltpu.VMEM((2, ny, ny), BF16),
            pltpu.VMEM((2, nz, nz), BF16),
            pltpu.SMEM((fields, fields), F32),
            pltpu.VMEM((1, nx), F32),
            pltpu.SMEM((ny,), F32),
            pltpu.VMEM((1, nz), F32),
            pltpu.VMEM((fields, n_py, rows_y, share_x), F32),
            pltpu.VMEM((fields, depth_y, share_x), F32),
            pltpu.VMEM((fields, depth_y, share_x), F32),
            pltpu.VMEM((fields, depth_z, share_x), F32),
            pltpu.VMEM((fields - 1, depth_z, share_x), F32),
            pltpu.VMEM((depth_z, share_x), F32),
            pltpu.VMEM((2, depth_y, depth_y), BF16),
            pltpu.VMEM((2, depth_z, depth_z), BF16),
            pltpu.SemaphoreType.DMA((fields,)),
            pltpu.SemaphoreType.DMA((8,)),
            pltpu.SemaphoreType.DMA((fields, n_py)),
            pltpu.SemaphoreType.DMA((fields, n_py)),
            pltpu.SemaphoreType.DMA((fields, n_pz)),
            pltpu.SemaphoreType.DMA((fields, n_pz)),
        ],
        compiler_params=pltpu.CompilerParams(
            collective_id=0, has_side_effects=True, vmem_limit_bytes=54500000
        ),
    )(
        values,
        jnp.asarray(split_table(nx)),
        jnp.asarray(split_table(ny)),
        jnp.asarray(split_table(nz)),
        coupling,
        symbol_x.reshape(1, nx),
        symbol_y,
        symbol_z.reshape(1, nz),
    )
    return jnp.transpose(out.reshape(fields, share_y, nz, share_x), (0, 3, 1, 2))


def solution(mesh):
    return jax.shard_map(
        functools.partial(shards, mesh.shape["py"], mesh.shape["pz"]),
        mesh=mesh,
        in_specs=(P(None, None, "py", "pz"), P(), P(), P(), P()),
        out_specs=P(None, "py", "pz", None),
        check_vma=False,
    )
```
